32 devices in a mesh: groups: 2 (over y), seq: 16 (over z, x, core).
Axes of the slice: x: 2, y: 2, z: 4, core: 2. Of those that a mesh axis runs over, the one named last changes fastest.
Arguments:
- query_rows: bfloat16 [2048, 2048], P(('groups', 'seq')), parts along dimension 0, may hold values from -180 to 180
- key_rows: bfloat16 [2048, 512], P(('groups', 'seq')), parts along dimension 0, may hold values from -6 to 6
- value_rows: bfloat16 [2048, 512], P(('groups', 'seq')), parts along dimension 0, may hold values from -6 to 6
- positions: int32 [2048], P(('groups', 'seq')), parts along dimension 0, may hold values from 0 to 1023, as said below
- prompt_length: int32 [2], P('groups'), parts along dimension 0, may hold values from 512 to 1024
- out_weight: bfloat16 [2048, 2048], replicated, may hold values from -0.125 to 0.125
- residual: bfloat16 [2048, 2048], P(('groups', 'seq')), parts along dimension 0, may hold values from -0.59765625 to 0.59765625
Outputs:
- layer_out: bfloat16 [2048, 2048], P(('groups', 'seq')), parts along dimension 0
The draws below stay inside these ranges and needn't reach their ends.
There are 2 independent parts, one for each index of `groups`. The reference program is written for one: setup_inputs(seed, part) draws one part's arguments, and reference() takes and returns one part's arrays. A program takes and returns all parts, laid end to end along the dimension named above; an argument that names none is the same for every part. Nothing has to cross between parts.
Inputs may be any that keep to these rules, and one draw needn't show every extreme that they name: A permutation of 0 to 1023 in which each device's rows hold exactly one position of every run of 16 consecutive positions.
All inputs are finite; a program needn't handle non-finite values.
Results may differ from the reference program's by a relative error of at most 0.009.
Values may be sent and summed in bfloat16 or wider, within the bound.
A program may use at most 128 MiB of HBM per device.

```python
import math
import jax
import jax.numpy as jnp
from jax import lax

HEADS = 16
KV_HEADS = 4
HEAD_DIM = 128
OUT_FEAT = 2048
TOK_DEV = 64
ATTN = 2048
LEN = 1024
N_SEQ = 16


def pair_draw(key):
    base = jax.random.fold_in(key, 41)
    seed_query, seed_key = jax.random.split(base, 2)
    group_size = HEADS // KV_HEADS
    key_vals = jnp.clip(jax.random.normal(seed_key, (LEN, KV_HEADS, HEAD_DIM), jnp.float32), -6.0, 6.0)
    query_vals = jnp.clip(jax.random.normal(seed_query, (LEN, KV_HEADS, group_size, HEAD_DIM), jnp.float32), -6.0, 6.0)
    return (query_vals.reshape(LEN, HEADS * HEAD_DIM), key_vals.reshape(LEN, KV_HEADS * HEAD_DIM))


def draw_query_rows(key, part):
    return pair_draw(key)[0].astype(jnp.bfloat16)


def draw_key_rows(key, part):
    return pair_draw(key)[1].astype(jnp.bfloat16)


def draw_positions(key, part):
    device_order = jax.random.permutation(jax.random.fold_in(key, 5), N_SEQ)
    row_index = jnp.arange(LEN, dtype=jnp.int32)
    return (row_index % TOK_DEV * N_SEQ + device_order[row_index // TOK_DEV]).astype(jnp.int32)


def block_levels(rng, dims, shards, least, high):
    def one(axis_at, shards_of):
        heights = jax.random.uniform(jax.random.fold_in(jax.random.fold_in(rng, 6), axis_at), (shards_of,), jnp.float32, least / len(shards), high / len(shards))
        return jnp.repeat(jnp.exp(heights), dims[axis_at] // shards_of).reshape((-1,) + (1,) * (len(dims) - axis_at - 1))

    factor_of = one(*shards[0])
    for cut in shards[1:]:
        factor_of = factor_of * one(*cut)
    return factor_of


def bell_draw(stream_key, extent, width, limit, cuts=(), held_as=jnp.bfloat16):
    entries = jax.random.normal(stream_key, extent, jnp.float32) * width
    if len(cuts) > 0:
        entries = block_levels(stream_key, extent, cuts, -0.22, 0.18) * entries
    return jnp.clip(entries, min=-limit, max=limit).astype(held_as)


def setup_inputs(seed: int = 0, part: int = 0) -> dict:
    key_of = jax.random.split(jax.random.key(seed), 8)
    part_splits = jax.random.split(jax.random.fold_in(key_of[7], part), 8)
    return {
        "query_rows": draw_query_rows(jax.random.fold_in(jax.random.fold_in(key_of[7], part), 71), part),
        "key_rows": draw_key_rows(jax.random.fold_in(jax.random.fold_in(key_of[7], part), 71), part),
        "value_rows": bell_draw(part_splits[2], (LEN, KV_HEADS * HEAD_DIM), 1.0, 6.0, ((0, 16),)),
        "positions": draw_positions(jax.random.fold_in(jax.random.fold_in(key_of[7], part), 71), part),
        "prompt_length": jax.random.randint(part_splits[4], (1,), LEN // 2, LEN + 1).astype(jnp.int32),
        "out_weight": bell_draw(key_of[5], (ATTN, OUT_FEAT), ATTN ** -0.5, 0.125),
        "residual": bell_draw(part_splits[6], (LEN, OUT_FEAT), 0.1, 0.59765625, ((0, 16),)),
    }


def reference(query_rows, key_rows, value_rows, positions, prompt_length, out_weight, residual):
    group_size = HEADS // KV_HEADS
    key_all = key_rows.reshape(LEN, KV_HEADS, HEAD_DIM).astype(jnp.float32)
    value_all = value_rows.reshape(LEN, KV_HEADS, HEAD_DIM).astype(jnp.float32)
    prompt_limit = prompt_length[0]
    block_rows = math.gcd(LEN, 512)
    block_count = LEN // block_rows
    query_blocks = query_rows.reshape(block_count, block_rows, KV_HEADS, group_size, HEAD_DIM)
    position_blocks = positions.reshape(block_count, block_rows)

    def attend(inputs):
        query_part, query_pos = inputs
        scores = jnp.einsum("qhgd,khd->hgqk", query_part.astype(jnp.float32), key_all) * HEAD_DIM ** -0.5
        visible = (positions[None, :] <= query_pos[:, None]) & (positions[None, :] < prompt_limit)
        scores = jnp.where(visible[None, None], scores, -1e30)
        maxima = jnp.max(scores, axis=-1, keepdims=True)
        weights = jnp.where(visible[None, None], jnp.exp(scores - maxima), 0.0)
        totals = jnp.sum(weights, axis=-1)
        rounded = lax.optimization_barrier(weights.astype(jnp.bfloat16))
        numerators = jnp.einsum("hgqk,khd->hgqd", rounded.astype(jnp.float32), value_all)
        attended = numerators / totals[..., None]
        return attended.transpose(2, 0, 1, 3).reshape(block_rows, HEADS * HEAD_DIM).astype(jnp.bfloat16)

    attended = lax.map(attend, (query_blocks, position_blocks)).reshape(LEN, HEADS * HEAD_DIM)
    projected = jnp.dot(attended, out_weight, preferred_element_type=jnp.float32)
    return (projected + residual.astype(jnp.float32)).astype(jnp.bfloat16)
```

```python
import functools
import math

import jax
import jax.numpy as jnp
from jax import lax
from jax.experimental import pallas as pl
from jax.experimental.pallas import tpu as pltpu
from jax.sharding import PartitionSpec as P

HEAD_DIM = 128
HEADS = 16
KV_HEADS = 4
UNROLLED_DEVICES = 32


def split_chips(seq):
    chips = seq // 2
    x_size = 1
    while 2 * x_size * 2 * x_size <= chips:
        x_size *= 2
    return x_size, chips // x_size


def fused_kernel(
    seq, x_size, z_size, kv_heads,
    limit_ref, pos_ref, query_hbm, key_hbm, value_hbm, weight_hbm, residual_hbm,
    out_ref,
    kv, pos_all, query, weight, residual, bias, acc,
    load_sem, kv_sem, weight_sem, send_sem, recv_sem, pos_send, pos_recv,
):
    tokens = query.shape[0]
    group = query.shape[1] // (kv_heads * HEAD_DIM)
    feat = group * HEAD_DIM
    keys = seq * tokens
    me = lax.axis_index("seq")
    core = lax.rem(me, 2)
    x_at = lax.rem(me // 2, x_size)
    z_at = me // (2 * x_size)

    def index_of(z, x, c):
        return (z * x_size + x) * 2 + c

    z_peers = [index_of(lax.rem(z_at + d, z_size), x_at, core) for d in range(1, z_size)]
    x_ids = [lax.rem(x_at + d, x_size) for d in range(1, x_size)]
    x_peers = [index_of(z_at, x, core) for x in x_ids]
    other = index_of(z_at, x_at, 1 - core)
    peers = z_peers + x_peers + [other]

    local = []
    for g in range(kv_heads):
        cols = pl.ds(g * HEAD_DIM, HEAD_DIM)
        pair = [
            pltpu.make_async_copy(key_hbm.at[:, cols], kv.at[g, me, 0], kv_sem.at[g, 0]),
            pltpu.make_async_copy(value_hbm.at[:, cols], kv.at[g, me, 1], kv_sem.at[g, 1]),
        ]
        for copy in pair:
            copy.start()
        local.append(pair)

    barrier = pltpu.get_barrier_semaphore()
    for peer in peers:
        pl.semaphore_signal(
            barrier, inc=1, device_id={"seq": peer}, device_id_type=pl.DeviceIdType.MESH
        )
    load_q = pltpu.make_async_copy(query_hbm, query, load_sem.at[0])
    load_r = pltpu.make_async_copy(residual_hbm, residual, load_sem.at[1])
    load_q.start()
    load_r.start()
    load_w = []
    for g in range(kv_heads):
        rows = pl.ds(g * feat, feat)
        copy = pltpu.make_async_copy(weight_hbm.at[rows], weight.at[rows], weight_sem.at[g])
        copy.start()
        load_w.append(copy)
    pl.semaphore_wait(barrier, len(peers))

    sends = []
    counts = [0] * kv_heads

    def send(g, slot, peer):
        if g == 0:
            copy = pltpu.make_async_remote_copy(
                src_ref=pos_all.at[slot], dst_ref=pos_all.at[slot],
                send_sem=pos_send.at[counts[g]], recv_sem=pos_recv.at[slot],
                device_id={"seq": peer}, device_id_type=pl.DeviceIdType.MESH,
            ) if slot is not me else pltpu.make_async_remote_copy(
                src_ref=pos_ref, dst_ref=pos_all.at[slot],
                send_sem=pos_send.at[counts[g]], recv_sem=pos_recv.at[slot],
                device_id={"seq": peer}, device_id_type=pl.DeviceIdType.MESH,
            )
            copy.start()
            sends.append(copy)
        copy = pltpu.make_async_remote_copy(
            src_ref=kv.at[g, slot], dst_ref=kv.at[g, slot],
            send_sem=send_sem.at[g, counts[g]], recv_sem=recv_sem.at[g, slot],
            device_id={"seq": peer}, device_id_type=pl.DeviceIdType.MESH,
        )
        copy.start()
        sends.append(copy)
        counts[g] += 1

    def arrive(g, slot):
        if g == 0:
            pltpu.make_async_remote_copy(
                src_ref=pos_all.at[slot], dst_ref=pos_all.at[slot],
                send_sem=pos_send.at[0], recv_sem=pos_recv.at[slot],
                device_id={"seq": other}, device_id_type=pl.DeviceIdType.MESH,
            ).wait_recv()
        pltpu.make_async_remote_copy(
            src_ref=kv.at[g, slot], dst_ref=kv.at[g, slot],
            send_sem=send_sem.at[g, 0], recv_sem=recv_sem.at[g, slot],
            device_id={"seq": other}, device_id_type=pl.DeviceIdType.MESH,
        ).wait_recv()

    z_slots = z_peers
    x_slots = [
        index_of(lax.rem(z_at + d, z_size), x, core) for d in range(z_size) for x in x_ids
    ]
    d_slots = [other]
    d_slots += [index_of(lax.rem(z_at + d, z_size), x_at, 1 - core) for d in range(1, z_size)]
    d_slots += [
        index_of(lax.rem(z_at + d, z_size), x, 1 - core) for d in range(z_size) for x in x_ids
    ]

    for g in range(kv_heads):
        for copy in local[g]:
            copy.wait()
        for peer in z_peers + x_peers + [other]:
            send(g, me, peer)

    def forward_z(g):
        for slot in z_slots:
            arrive(g, slot)
            for peer in x_peers:
                send(g, slot, peer)
            send(g, slot, other)

    def forward_x(g):
        for slot in x_slots:
            arrive(g, slot)
            send(g, slot, other)

    def receive(g):
        for slot in d_slots:
            arrive(g, slot)

    def make_bias():
        own = pos_ref[...]
        pos_all[me] = own
        square = jnp.broadcast_to(own, (tokens, tokens))
        diag = lax.broadcasted_iota(jnp.int32, (tokens, tokens), 0) == (
            lax.broadcasted_iota(jnp.int32, (tokens, tokens), 1)
        )
        column = jnp.sum(jnp.where(diag, square, 0), axis=1, keepdims=True)
        cut = jnp.minimum(column, limit_ref[0] - 1)
        row = jnp.concatenate([pos_all[s] for s in range(seq)], axis=1)
        bias[...] = jnp.where(row <= cut, 0.0, -1e30)

    def compute(g):
        q = jnp.concatenate(
            [query[:, (g * group + i) * HEAD_DIM:(g * group + i + 1) * HEAD_DIM] for i in range(group)],
            axis=0,
        )
        k = kv[g, :, 0].reshape(keys, HEAD_DIM)
        v = kv[g, :, 1].reshape(keys, HEAD_DIM)
        s = lax.dot_general(q, k, (((1,), (1,)), ((), ())), preferred_element_type=jnp.float32)
        s = s.reshape(group, tokens, keys) * (HEAD_DIM ** -0.5 * math.log2(math.e)) + bias[...][None]
        s = s.reshape(group * tokens, keys)
        p = jnp.exp2(s - jnp.max(s, axis=1, keepdims=True))
        total = jnp.sum(p, axis=1, keepdims=True)
        o = jnp.dot(p.astype(jnp.bfloat16), v, preferred_element_type=jnp.float32)
        o = (o / total).astype(jnp.bfloat16)
        a = jnp.concatenate([o[i * tokens:(i + 1) * tokens] for i in range(group)], axis=1)
        load_w[g].wait()
        part = jnp.dot(a, weight[g * feat:(g + 1) * feat, :], preferred_element_type=jnp.float32)
        if g == 0:
            load_r.wait()
            acc[...] = part + residual[...].astype(jnp.float32)
        elif g < kv_heads - 1:
            acc[...] += part
        else:
            out_ref[...] = (acc[...] + part).astype(jnp.bfloat16)

    forward_z(0)
    load_q.wait()
    for g in range(kv_heads):
        if g + 1 < kv_heads:
            forward_z(g + 1)
        forward_x(g)
        receive(g)
        if g == 0:
            make_bias()
        if g == kv_heads - 1:
            for copy in sends:
                copy.wait_send()
        compute(g)


def fused(seq, query_rows, key_rows, value_rows, positions, prompt_length, out_weight, residual):
    x_size, z_size = split_chips(seq)
    tokens = query_rows.shape[0]
    kv_heads = key_rows.shape[1] // HEAD_DIM
    steps = (z_size - 1) * (x_size + 1) + x_size + (x_size - 1) * z_size
    hbm = pl.BlockSpec(memory_space=pl.ANY)
    vmem = pl.BlockSpec(memory_space=pltpu.VMEM)
    return pl.pallas_call(
        functools.partial(fused_kernel, seq, x_size, z_size, kv_heads),
        out_shape=jax.ShapeDtypeStruct(residual.shape, jnp.bfloat16),
        in_specs=[pl.BlockSpec(memory_space=pltpu.SMEM), vmem, hbm, hbm, hbm, hbm, hbm],
        out_specs=vmem,
        scratch_shapes=[
            pltpu.VMEM((kv_heads, seq, 2, tokens, HEAD_DIM), jnp.bfloat16),
            pltpu.VMEM((seq, 1, tokens), jnp.int32),
            pltpu.VMEM(query_rows.shape, jnp.bfloat16),
            pltpu.VMEM(out_weight.shape, jnp.bfloat16),
            pltpu.VMEM(residual.shape, jnp.bfloat16),
            pltpu.VMEM((tokens, seq * tokens), jnp.float32),
            pltpu.VMEM(residual.shape, jnp.float32),
            pltpu.SemaphoreType.DMA((2,)),
            pltpu.SemaphoreType.DMA((kv_heads, 2)),
            pltpu.SemaphoreType.DMA((kv_heads,)),
            pltpu.SemaphoreType.DMA((kv_heads, steps + z_size)),
            pltpu.SemaphoreType.DMA((kv_heads, seq)),
            pltpu.SemaphoreType.DMA((steps + z_size,)),
            pltpu.SemaphoreType.DMA((seq,)),
        ],
        compiler_params=pltpu.CompilerParams(
            collective_id=0, has_side_effects=True, vmem_limit_bytes=60 * 1024 * 1024
        ),
    )(prompt_length, positions.reshape(1, tokens), query_rows, key_rows, value_rows, out_weight, residual)


def largest_block(total_rows):
    size_now = min(total_rows, 1024)
    while total_rows % size_now:
        size_now -= 1
    return size_now


def attend_block(state_now, key_part, value_part, key_pos, queries, query_pos, prompt_limit):
    maxima, totals, numerators = state_now
    scores = jnp.einsum(
        "hqd,khd->hqk", queries, key_part, preferred_element_type=jnp.float32
    ) * HEAD_DIM ** (-0.5)
    visible = (key_pos[None, None, :] <= query_pos[None, :, None]) & (
        key_pos[None, None, :] < prompt_limit
    )
    scores = jnp.where(visible, scores, -1e30)
    new_max = jnp.maximum(maxima, jnp.max(scores, axis=-1))
    weights = jnp.where(visible, jnp.exp(scores - new_max[..., None]), 0.0)
    rescale = jnp.exp(maxima - new_max)
    totals = totals * rescale + jnp.sum(weights, axis=-1)
    numerators = numerators * rescale[..., None] + jnp.einsum(
        "hqk,khd->hqd", weights.astype(jnp.bfloat16), value_part, preferred_element_type=jnp.float32
    )
    return (new_max, totals, numerators)


def sweep(state_now, key_block, value_block, key_pos, queries, query_pos, prompt_limit):
    total_rows = key_block.shape[0]
    width_rows = largest_block(total_rows)
    key_part = key_block.reshape(total_rows, KV_HEADS, HEAD_DIM)
    value_part = value_block.reshape(total_rows, KV_HEADS, HEAD_DIM)
    if width_rows == total_rows:
        return attend_block(
            state_now, key_part, value_part, key_pos, queries, query_pos, prompt_limit
        )
    count_blocks = total_rows // width_rows
    stacked = (
        key_part.reshape(count_blocks, width_rows, KV_HEADS, HEAD_DIM),
        value_part.reshape(count_blocks, width_rows, KV_HEADS, HEAD_DIM),
        key_pos.reshape(count_blocks, width_rows),
    )

    def step_block(state_in, blocks):
        return (
            attend_block(
                state_in, blocks[0], blocks[1], blocks[2], queries, query_pos, prompt_limit
            ),
            None,
        )

    state_out, unused = lax.scan(step_block, state_now, stacked)
    return state_out


def streamed(query_rows, key_rows, value_rows, positions, prompt_length, out_weight, residual):
    tokens_here = query_rows.shape[0]
    group_size = HEADS // KV_HEADS
    queries = query_rows.reshape(tokens_here, KV_HEADS, group_size, HEAD_DIM).transpose(1, 2, 0, 3)
    queries = queries.reshape(KV_HEADS, group_size * tokens_here, HEAD_DIM)
    query_pos = jnp.tile(positions, group_size)
    prompt_limit = prompt_length[0]
    start_state = (
        jnp.full((KV_HEADS, group_size * tokens_here), -1e30, jnp.float32),
        jnp.zeros((KV_HEADS, group_size * tokens_here), jnp.float32),
        jnp.zeros((KV_HEADS, group_size * tokens_here, HEAD_DIM), jnp.float32),
    )
    final_state = sweep(
        start_state,
        lax.all_gather(key_rows, "seq", axis=0, tiled=True),
        lax.all_gather(value_rows, "seq", axis=0, tiled=True),
        lax.all_gather(positions, "seq", axis=0, tiled=True),
        queries,
        query_pos,
        prompt_limit,
    )
    maxima, totals, numerators = final_state
    attended = (numerators / totals[..., None]).reshape(KV_HEADS, group_size, tokens_here, HEAD_DIM)
    attended = (
        attended.transpose(2, 0, 1, 3).reshape(tokens_here, HEADS * HEAD_DIM).astype(jnp.bfloat16)
    )
    projected = jnp.dot(attended, out_weight, preferred_element_type=jnp.float32)
    return (projected + residual.astype(jnp.float32)).astype(jnp.bfloat16)


def on_device(seq, *arrays):
    if seq <= UNROLLED_DEVICES:
        return fused(seq, *arrays)
    return streamed(*arrays)


def solution(mesh):
    return jax.shard_map(
        functools.partial(on_device, mesh.shape["seq"]),
        mesh=mesh,
        in_specs=(
            P(("groups", "seq"), None),
            P(("groups", "seq"), None),
            P(("groups", "seq"), None),
            P(("groups", "seq")),
            P("groups"),
            P(),
            P(("groups", "seq"), None),
        ),
        out_specs=P(("groups", "seq"), None),
        check_vma=False,
    )
```

```python
import functools
import math

import jax
import jax.numpy as jnp
from jax import lax
from jax.experimental import pallas as pl
from jax.experimental.pallas import tpu as pltpu
from jax.sharding import PartitionSpec as P

HEAD_DIM = 128
HEADS = 16
KV_HEADS = 4


def split_chips(seq):
    chips = seq // 2
    x_size = 1
    while 2 * x_size * 2 * x_size <= chips:
        x_size *= 2
    return x_size, chips // x_size


def fused_kernel(
    seq, x_size, z_size, kv_heads,
    limit_ref, pos_ref, query_hbm, key_hbm, value_hbm, weight_hbm, residual_hbm,
    out_ref,
    kv, pos_all, query, weight, residual, bias, acc,
    load_sem, kv_sem, weight_sem, send_sem, recv_sem, pos_send, pos_recv,
):
    tokens = query.shape[0]
    group = query.shape[1] // (kv_heads * HEAD_DIM)
    feat = group * HEAD_DIM
    keys = seq * tokens
    me = lax.axis_index("seq")
    core = lax.rem(me, 2)
    x_at = lax.rem(me // 2, x_size)
    z_at = me // (2 * x_size)

    def index_of(z, x, c):
        return (z * x_size + x) * 2 + c

    z_peers = [index_of(lax.rem(z_at + d, z_size), x_at, core) for d in range(1, z_size)]
    x_ids = [lax.rem(x_at + d, x_size) for d in range(1, x_size)]
    x_peers = [index_of(z_at, x, core) for x in x_ids]
    other = index_of(z_at, x_at, 1 - core)
    z_near = z_at + 1 - 2 * lax.rem(z_at, 2)
    z_far = [lax.rem(z + 2, 4) for z in (z_at, z_near)]
    near = index_of(z_near, x_at, core)
    z_rest = [index_of(z, x_at, core) for z in z_far]
    x_peer = x_peers[0]
    x_rest = [index_of(z, 1 - x_at, core) for z in (z_near, *z_far)]
    peers = z_peers + x_peers + [other]

    local = []
    for g in range(kv_heads):
        cols = pl.ds(g * HEAD_DIM, HEAD_DIM)
        pair = [
            pltpu.make_async_copy(key_hbm.at[:, cols], kv.at[g, me, 0], kv_sem.at[g, 0]),
            pltpu.make_async_copy(value_hbm.at[:, cols], kv.at[g, me, 1], kv_sem.at[g, 1]),
        ]
        for copy in pair:
            copy.start()
        local.append(pair)

    barrier = pltpu.get_barrier_semaphore()
    for peer in peers:
        pl.semaphore_signal(
            barrier, inc=1, device_id={"seq": peer}, device_id_type=pl.DeviceIdType.MESH
        )
    load_q = pltpu.make_async_copy(query_hbm, query, load_sem.at[0])
    load_r = pltpu.make_async_copy(residual_hbm, residual, load_sem.at[1])
    load_q.start()
    load_r.start()
    load_w = []
    for g in range(kv_heads):
        rows = pl.ds(g * feat, feat)
        copy = pltpu.make_async_copy(weight_hbm.at[rows], weight.at[rows], weight_sem.at[g])
        copy.start()
        load_w.append(copy)
    pl.semaphore_wait(barrier, len(peers))

    sends = []
    counts = [0] * kv_heads

    def send(g, slot, peer):
        if g == 0:
            copy = pltpu.make_async_remote_copy(
                src_ref=pos_all.at[slot], dst_ref=pos_all.at[slot],
                send_sem=pos_send.at[counts[g]], recv_sem=pos_recv.at[slot],
                device_id={"seq": peer}, device_id_type=pl.DeviceIdType.MESH,
            ) if slot is not me else pltpu.make_async_remote_copy(
                src_ref=pos_ref, dst_ref=pos_all.at[slot],
                send_sem=pos_send.at[counts[g]], recv_sem=pos_recv.at[slot],
                device_id={"seq": peer}, device_id_type=pl.DeviceIdType.MESH,
            )
            copy.start()
            sends.append(copy)
        copy = pltpu.make_async_remote_copy(
            src_ref=kv.at[g, slot], dst_ref=kv.at[g, slot],
            send_sem=send_sem.at[g, counts[g]], recv_sem=recv_sem.at[g, slot],
            device_id={"seq": peer}, device_id_type=pl.DeviceIdType.MESH,
        )
        copy.start()
        sends.append(copy)
        counts[g] += 1

    def arrive(g, slot):
        if g == 0:
            pltpu.make_async_remote_copy(
                src_ref=pos_all.at[slot], dst_ref=pos_all.at[slot],
                send_sem=pos_send.at[0], recv_sem=pos_recv.at[slot],
                device_id={"seq": other}, device_id_type=pl.DeviceIdType.MESH,
            ).wait_recv()
        pltpu.make_async_remote_copy(
            src_ref=kv.at[g, slot], dst_ref=kv.at[g, slot],
            send_sem=send_sem.at[g, 0], recv_sem=recv_sem.at[g, slot],
            device_id={"seq": other}, device_id_type=pl.DeviceIdType.MESH,
        ).wait_recv()

    z_slots = z_peers
    x_slots = [
        index_of(lax.rem(z_at + d, z_size), x, core) for d in range(z_size) for x in x_ids
    ]
    d_slots = [other]
    d_slots += [index_of(lax.rem(z_at + d, z_size), x_at, 1 - core) for d in range(1, z_size)]
    d_slots += [
        index_of(lax.rem(z_at + d, z_size), x, 1 - core) for d in range(z_size) for x in x_ids
    ]

    for g in range(kv_heads):
        for copy in local[g]:
            copy.wait()
        for peer in z_peers + x_peers + [other]:
            send(g, me, peer)

    def relay(g, slot, *to):
        arrive(g, slot)
        for peer in to:
            send(g, slot, peer)

    def forward_z(g):
        swap = g % 2 == 1
        relay(g, x_peer, *((near, other) if swap else (other,)))
        relay(g, near, *((other,) if swap else (x_peer, other)))
        for slot in z_rest:
            relay(g, slot, x_peer, other)

    def forward_x(g):
        for slot in x_rest:
            relay(g, slot, other)

    def receive(g):
        for slot in d_slots:
            arrive(g, slot)

    def make_bias():
        own = pos_ref[...]
        pos_all[me] = own
        square = jnp.broadcast_to(own, (tokens, tokens))
        diag = lax.broadcasted_iota(jnp.int32, (tokens, tokens), 0) == (
            lax.broadcasted_iota(jnp.int32, (tokens, tokens), 1)
        )
        column = jnp.sum(jnp.where(diag, square, 0), axis=1, keepdims=True)
        cut = jnp.minimum(column, limit_ref[0] - 1)
        row = jnp.concatenate([pos_all[s] for s in range(seq)], axis=1)
        bias[...] = jnp.where(row <= cut, 0.0, -1e30)

    def compute(g):
        q = jnp.concatenate(
            [query[:, (g * group + i) * HEAD_DIM:(g * group + i + 1) * HEAD_DIM] for i in range(group)],
            axis=0,
        )
        k = kv[g, :, 0].reshape(keys, HEAD_DIM)
        v = kv[g, :, 1].reshape(keys, HEAD_DIM)
        s = lax.dot_general(q, k, (((1,), (1,)), ((), ())), preferred_element_type=jnp.float32)
        s = s.reshape(group, tokens, keys) * (HEAD_DIM ** -0.5 * math.log2(math.e)) + bias[...][None]
        s = s.reshape(group * tokens, keys)
        p = jnp.exp2(s - jnp.max(s, axis=1, keepdims=True))
        total = jnp.sum(p, axis=1, keepdims=True)
        o = jnp.dot(p.astype(jnp.bfloat16), v, preferred_element_type=jnp.float32)
        o = (o / total).astype(jnp.bfloat16)
        a = jnp.concatenate([o[i * tokens:(i + 1) * tokens] for i in range(group)], axis=1)
        load_w[g].wait()
        part = jnp.dot(a, weight[g * feat:(g + 1) * feat, :], preferred_element_type=jnp.float32)
        if g == 0:
            load_r.wait()
            acc[...] = part + residual[...].astype(jnp.float32)
        elif g < kv_heads - 1:
            acc[...] += part
        else:
            out_ref[...] = (acc[...] + part).astype(jnp.bfloat16)

    def finish(g):
        receive(g)
        if g == 0:
            load_q.wait()
            make_bias()
        if g == kv_heads - 1:
            for copy in sends:
                copy.wait_send()
        compute(g)

    stages = {"z": forward_z, "x": forward_x, "c": finish}
    for step in 'z0 z1 x0 z2 x1 c0 z3 x2 c1 x3 c2 c3'.split():
        stages[step[0]](int(step[1:]))


def fused(seq, query_rows, key_rows, value_rows, positions, prompt_length, out_weight, residual):
    x_size, z_size = split_chips(seq)
    tokens = query_rows.shape[0]
    kv_heads = key_rows.shape[1] // HEAD_DIM
    steps = (z_size - 1) * (x_size + 1) + x_size + (x_size - 1) * z_size
    hbm = pl.BlockSpec(memory_space=pl.ANY)
    vmem = pl.BlockSpec(memory_space=pltpu.VMEM)
    return pl.pallas_call(
        functools.partial(fused_kernel, seq, x_size, z_size, kv_heads),
        out_shape=pltpu.VMEM(residual.shape, jnp.bfloat16),
        in_specs=[pl.BlockSpec(memory_space=pltpu.SMEM), vmem, hbm, hbm, hbm, hbm, hbm],
        out_specs=pl.BlockSpec(memory_space=pltpu.VMEM),
        scratch_shapes=[
            pltpu.VMEM((kv_heads, seq, 2, tokens, HEAD_DIM), jnp.bfloat16),
            pltpu.VMEM((seq, 1, tokens), jnp.int32),
            pltpu.VMEM(query_rows.shape, jnp.bfloat16),
            pltpu.VMEM(out_weight.shape, jnp.bfloat16),
            pltpu.VMEM(residual.shape, jnp.bfloat16),
            pltpu.VMEM((tokens, seq * tokens), jnp.float32),
            pltpu.VMEM(residual.shape, jnp.float32),
            pltpu.SemaphoreType.DMA((2,)),
            pltpu.SemaphoreType.DMA((kv_heads, 2)),
            pltpu.SemaphoreType.DMA((kv_heads,)),
            pltpu.SemaphoreType.DMA((kv_heads, steps + z_size)),
            pltpu.SemaphoreType.DMA((kv_heads, seq)),
            pltpu.SemaphoreType.DMA((steps + z_size,)),
            pltpu.SemaphoreType.DMA((seq,)),
        ],
        compiler_params=pltpu.CompilerParams(
            collective_id=0, has_side_effects=True, vmem_limit_bytes=60 * 1024 * 1024
        ),
    )(prompt_length, positions.reshape(1, tokens), query_rows, key_rows, value_rows, out_weight, residual)


def largest_block(total_rows):
    size_now = min(total_rows, 1024)
    while total_rows % size_now:
        size_now -= 1
    return size_now


def attend_block(state_now, key_part, value_part, key_pos, queries, query_pos, prompt_limit):
    maxima, totals, numerators = state_now
    scores = jnp.einsum(
        "hqd,khd->hqk", queries, key_part, preferred_element_type=jnp.float32
    ) * HEAD_DIM ** (-0.5)
    visible = (key_pos[None, None, :] <= query_pos[None, :, None]) & (
        key_pos[None, None, :] < prompt_limit
    )
    scores = jnp.where(visible, scores, -1e30)
    new_max = jnp.maximum(maxima, jnp.max(scores, axis=-1))
    weights = jnp.where(visible, jnp.exp(scores - new_max[..., None]), 0.0)
    rescale = jnp.exp(maxima - new_max)
    totals = totals * rescale + jnp.sum(weights, axis=-1)
    numerators = numerators * rescale[..., None] + jnp.einsum(
        "hqk,khd->hqd", weights.astype(jnp.bfloat16), value_part, preferred_element_type=jnp.float32
    )
    return (new_max, totals, numerators)


def sweep(state_now, key_block, value_block, key_pos, queries, query_pos, prompt_limit):
    total_rows = key_block.shape[0]
    width_rows = largest_block(total_rows)
    key_part = key_block.reshape(total_rows, KV_HEADS, HEAD_DIM)
    value_part = value_block.reshape(total_rows, KV_HEADS, HEAD_DIM)
    if width_rows == total_rows:
        return attend_block(
            state_now, key_part, value_part, key_pos, queries, query_pos, prompt_limit
        )
    count_blocks = total_rows // width_rows
    stacked = (
        key_part.reshape(count_blocks, width_rows, KV_HEADS, HEAD_DIM),
        value_part.reshape(count_blocks, width_rows, KV_HEADS, HEAD_DIM),
        key_pos.reshape(count_blocks, width_rows),
    )

    def step_block(state_in, blocks):
        return (
            attend_block(
                state_in, blocks[0], blocks[1], blocks[2], queries, query_pos, prompt_limit
            ),
            None,
        )

    state_out, unused = lax.scan(step_block, state_now, stacked)
    return state_out


def streamed(query_rows, key_rows, value_rows, positions, prompt_length, out_weight, residual):
    tokens_here = query_rows.shape[0]
    group_size = HEADS // KV_HEADS
    queries = query_rows.reshape(tokens_here, KV_HEADS, group_size, HEAD_DIM).transpose(1, 2, 0, 3)
    queries = queries.reshape(KV_HEADS, group_size * tokens_here, HEAD_DIM)
    query_pos = jnp.tile(positions, group_size)
    prompt_limit = prompt_length[0]
    start_state = (
        jnp.full((KV_HEADS, group_size * tokens_here), -1e30, jnp.float32),
        jnp.zeros((KV_HEADS, group_size * tokens_here), jnp.float32),
        jnp.zeros((KV_HEADS, group_size * tokens_here, HEAD_DIM), jnp.float32),
    )
    final_state = sweep(
        start_state,
        lax.all_gather(key_rows, "seq", axis=0, tiled=True),
        lax.all_gather(value_rows, "seq", axis=0, tiled=True),
        lax.all_gather(positions, "seq", axis=0, tiled=True),
        queries,
        query_pos,
        prompt_limit,
    )
    maxima, totals, numerators = final_state
    attended = (numerators / totals[..., None]).reshape(KV_HEADS, group_size, tokens_here, HEAD_DIM)
    attended = (
        attended.transpose(2, 0, 1, 3).reshape(tokens_here, HEADS * HEAD_DIM).astype(jnp.bfloat16)
    )
    projected = jnp.dot(attended, out_weight, preferred_element_type=jnp.float32)
    return (projected + residual.astype(jnp.float32)).astype(jnp.bfloat16)


def on_device(seq, *arrays):
    if split_chips(seq) == (2, 4):
        return fused(seq, *arrays)
    return streamed(*arrays)


def solution(mesh):
    return jax.shard_map(
        functools.partial(on_device, mesh.shape["seq"]),
        mesh=mesh,
        in_specs=(
            P(("groups", "seq"), None),
            P(("groups", "seq"), None),
            P(("groups", "seq"), None),
            P(("groups", "seq")),
            P("groups"),
            P(),
            P(("groups", "seq"), None),
        ),
        out_specs=P(("groups", "seq"), None),
        check_vma=False,
    )
```
